32 devices in a mesh: dp: 8 (over z, core), expert: 4 (over y, x).
Axes of the slice: x: 2, y: 2, z: 4, core: 2. Of those that a mesh axis runs over, the one named last changes fastest.
Arguments:
- attention_gradient: bfloat16 [8, 6144, 1024], P('dp', None, 'expert')
- attention_weight: float32 [6144, 1024], P('dp', 'expert'), may hold values from -6 to 6
- attention_mean: float32 [6144, 1024], P('dp', 'expert'), may hold values from -0.0012 to 0.0012
- attention_square: float32 [6144, 1024], P('dp', 'expert'), may hold values from 1e-09 to 1e-07
- expert_gradient: float32 [8, 4, 8, 6144], P('dp', 'expert')
- expert_weight: float32 [8, 4, 8, 6144], P('dp', 'expert'), may hold values from -6 to 6
- held_mean: float32 [8, 32, 6144], P('dp', 'expert'), may hold values from -0.0006 to 0.0006
- held_square: float32 [8, 32, 6144], P('dp', 'expert'), may hold values from 1e-10 to 1e-08
- live_block_count: int32 [4], replicated, may hold values from 1 to 8, as said below
- holder_table: int32 [4, 8], replicated, may hold values from 0 to 3, as said below
- slot_table: int32 [4, 8], replicated, may hold values from 0 to 7, as said below
- step_count: int32 [1], replicated, may hold values from 1 to 40
Outputs:
- updated_attention: float32 [6144, 1024], P('dp', 'expert')
- updated_means: float32 [6144, 1024], P('dp', 'expert')
- updated_squares: float32 [6144, 1024], P('dp', 'expert')
- updated_experts: float32 [8, 4, 8, 6144], P('dp', 'expert')
- expert_means: float32 [8, 4, 8, 6144], P('dp', 'expert')
- expert_squares: float32 [8, 4, 8, 6144], P('dp', 'expert')
The draws below stay inside these ranges and needn't reach their ends.
Inputs may be any that keep to these rules, and one draw needn't show every extreme that they name: `live_block_count`: every expert has 1 to 8 live blocks and some expert has exactly 8. `holder_table`: no holder holds more than 2 live blocks of one expert, and some holder holds exactly 2 of one. `slot_table`: the blocks on one holder sit in distinct slots, and some holder has all 8 slots live.
All inputs are finite; a program needn't handle non-finite values.
Results may differ from the reference program's by a relative error of at most 0.0003.
Values sent between devices are 32-bit elements; how exact they have to be, the bound alone decides.
A program may use at most 64 MiB of HBM per device.

```python
import math
import jax
import jax.numpy as jnp
from jax import lax

D = 6144
KV_COLS = 1024
MAXB = 8
HSLOTS = 8
CAP = 2
N_DP = 8
N_EXPERT = 4


def placement_tables(key):
    base = jax.random.fold_in(key, 7)
    key_order, key_turn, key_count = jax.random.split(base, 3)
    order = jax.random.permutation(key_order, N_EXPERT).astype(jnp.int32)
    turns = jax.random.randint(key_turn, (N_EXPERT,), 0, HSLOTS, dtype=jnp.int32)
    counts = jax.random.randint(key_count, (N_EXPERT,), 1, MAXB + 1, dtype=jnp.int32)
    floor_count = MAXB - order * CAP
    counts = jnp.where(order < MAXB // CAP, jnp.maximum(counts, floor_count), counts)
    block_position = jnp.arange(MAXB, dtype=jnp.int32)
    holders = ((order[:, None] + block_position[None, :] // CAP) % N_EXPERT).astype(jnp.int32)
    slots = ((block_position[None, :] + turns[holders]) % HSLOTS).astype(jnp.int32)
    return (counts.astype(jnp.int32), holders, slots)


def draw_live_block_count(key, part):
    return placement_tables(key)[0]


def draw_holder_table(key, part):
    return placement_tables(key)[1]


def draw_slot_table(key, part):
    return placement_tables(key)[2]


def draw_attention_gradient(key, part):
    key_noise, key_rows, key_cols, key_source = jax.random.split(key, 4)
    noise = jax.random.normal(key_noise, (N_DP, D, KV_COLS), jnp.float32)
    rising = jnp.power(3.0, jnp.arange(D, dtype=jnp.float32) / D)
    row_scale = rising * jnp.exp(jax.random.uniform(key_rows, (D,), jnp.float32, 0.0, math.log(3.4)))
    col_scale = jnp.exp(jax.random.uniform(key_cols, (KV_COLS,), jnp.float32, 0.0, math.log(3.0)))
    source = jnp.exp(jax.random.uniform(key_source, (N_DP, 1, 1), jnp.float32, math.log(0.5), math.log(2.0)))
    return (noise * source * row_scale[None, :, None] * col_scale[None, None, :]).astype(jnp.bfloat16)


def draw_expert_gradient(key, part):
    key_noise, key_blocks, key_cols = jax.random.split(key, 3)
    shape = (N_DP, N_EXPERT, MAXB, D)
    noise = jax.random.normal(key_noise, shape, jnp.float32)
    flat = jnp.arange(N_DP * N_EXPERT, dtype=jnp.float32).reshape(N_DP, N_EXPERT) / (N_DP * N_EXPERT)
    rising = jnp.power(3.0, flat)[:, :, None, None]
    block_scale = jnp.exp(jax.random.uniform(key_blocks, (N_DP, N_EXPERT, MAXB, 1), jnp.float32, 0.0, math.log(10.0)))
    col_scale = jnp.exp(jax.random.uniform(key_cols, (D,), jnp.float32, 0.0, math.log(3.0)))
    return noise * rising * block_scale * col_scale[None, None, None, :]


def levels(rng, dims, cuts, low, high):
    level = 1.0
    for position, blocks in cuts:
        draws = jax.random.uniform(jax.random.fold_in(jax.random.fold_in(rng, 6), position), (blocks,), jnp.float32, low / len(cuts), high / len(cuts))
        level = level * jnp.repeat(jnp.exp(draws), dims[position] // blocks).reshape((-1,) + (1,) * (len(dims) - 1 - position))
    return level


def bell_draw(key, extent, deviation, reach, cuts=(), kind=jnp.bfloat16):
    entries = deviation * jax.random.normal(key, extent, jnp.float32)
    if cuts:
        entries = entries * levels(key, extent, cuts, -0.22, 0.18)
    return jnp.clip(entries, -reach, reach).astype(kind)


def setup_inputs(seed: int = 0) -> dict:
    streams_of = jax.random.split(jax.random.key(seed), 13)
    attention_gradient = draw_attention_gradient(jax.random.fold_in(streams_of[12], 71), 0)
    attention_weight = bell_draw(streams_of[1], (D, KV_COLS), 1.0, 6.0, ((0, 8), (1, 4)), jnp.float32)
    attention_mean = bell_draw(streams_of[2], (D, KV_COLS), 0.0002, 0.0012, ((0, 8), (1, 4)), jnp.float32)
    attention_square = jnp.clip(jnp.exp(math.log(1.0000000116860974e-07) - 4.6051702 * jax.random.uniform(streams_of[3], (D, KV_COLS), jnp.float32) ** levels(streams_of[3], (D, KV_COLS), ((0, 8), (1, 4)), -0.2, 0.2)), 9.999999717180685e-10, 1.0000000116860974e-07)
    expert_gradient = draw_expert_gradient(jax.random.fold_in(streams_of[12], 71), 0)
    expert_weight = bell_draw(streams_of[5], (N_DP, N_EXPERT, MAXB, D), 1.0, 6.0, ((0, 8), (1, 4)), jnp.float32)
    held_mean = bell_draw(streams_of[6], (N_DP, N_EXPERT * HSLOTS, D), 0.0001, 0.0006, ((0, 8), (1, 4)), jnp.float32)
    held_square = jnp.clip(jnp.exp(math.log(9.99999993922529e-09) - 4.6051702 * jax.random.uniform(streams_of[7], (N_DP, N_EXPERT * HSLOTS, D), jnp.float32) ** levels(streams_of[7], (N_DP, N_EXPERT * HSLOTS, D), ((0, 8), (1, 4)), -0.2, 0.2)), 1.000000013351432e-10, 9.99999993922529e-09)
    live_block_count = draw_live_block_count(jax.random.fold_in(streams_of[12], 71), 0)
    holder_table = draw_holder_table(jax.random.fold_in(streams_of[12], 71), 0)
    slot_table = draw_slot_table(jax.random.fold_in(streams_of[12], 71), 0)
    step_count = jax.random.randint(streams_of[11], (1,), 1, 41).astype(jnp.int32)
    return dict(attention_gradient=attention_gradient, attention_weight=attention_weight, attention_mean=attention_mean, attention_square=attention_square, expert_gradient=expert_gradient, expert_weight=expert_weight, held_mean=held_mean, held_square=held_square, live_block_count=live_block_count, holder_table=holder_table, slot_table=slot_table, step_count=step_count)


beta_first = 0.9
beta_second = 0.95
learn_rate = 0.1
decay_rate = 0.1
adam_epsilon = 1e-08
clip_norm = 1.0

def adam_step(weight, mean, square, gradient, factor, step_float):
    scaled = factor * gradient
    mean_new = beta_first * mean + (1.0 - beta_first) * scaled
    square_new = beta_second * square + (1.0 - beta_second) * scaled * scaled
    mean_hat = mean_new / (1.0 - jnp.power(beta_first, step_float))
    square_hat = square_new / (1.0 - jnp.power(beta_second, step_float))
    weight_new = weight - learn_rate * (mean_hat / (jnp.sqrt(square_hat) + adam_epsilon) + decay_rate * weight)
    return (weight_new, mean_new, square_new)

def reference(attention_gradient, attention_weight, attention_mean, attention_square, expert_gradient, expert_weight, held_mean, held_square, live_block_count, holder_table, slot_table, step_count):

    def accumulate(running, piece):
        return (running + piece.astype(jnp.float32), None)
    summed, _ = lax.scan(accumulate, jnp.zeros(attention_gradient.shape[1:], jnp.float32), attention_gradient)
    block_position = jnp.arange(MAXB, dtype=jnp.int32)
    live_block_mask = (block_position[None, :] < live_block_count[:, None]).astype(jnp.float32)
    spread_blocks = live_block_mask[None, :, :, None]
    attention_part = jnp.sum(summed * summed)
    expert_share = jnp.sum(spread_blocks * expert_gradient * expert_gradient)
    total = attention_part + expert_share
    factor = jnp.minimum(1.0, clip_norm / (jnp.sqrt(total) + 1e-06))
    step_float = step_count[0].astype(jnp.float32)
    attention_new, means_new, squares_new = adam_step(attention_weight, attention_mean, attention_square, summed, factor, step_float)
    indices = (holder_table * HSLOTS + slot_table).astype(jnp.int32)
    owned_mean = held_mean[:, indices, :] * spread_blocks
    owned_square = held_square[:, indices, :] * spread_blocks
    weight_next, mean_next, square_next = adam_step(expert_weight, owned_mean, owned_square, expert_gradient, factor, step_float)
    live_flags = spread_blocks > 0.5
    experts_new = jnp.where(live_flags, weight_next, expert_weight)
    expert_means = jnp.where(live_flags, mean_next, 0.0)
    expert_squares = jnp.where(live_flags, square_next, 0.0)
    return (attention_new, means_new, squares_new, experts_new, expert_means, expert_squares)
```

```python
import functools

import jax
import jax.numpy as jnp
from jax import lax
from jax.experimental import pallas as pl
from jax.experimental.pallas import tpu as pltpu
from jax.sharding import PartitionSpec as P

MESH = pl.DeviceIdType.MESH
CORES = 2
LAG = 3

beta_first = 0.9
beta_second = 0.95
learn_rate = 0.1
decay_rate = 0.1
adam_epsilon = 1e-08
clip_norm = 1.0


def power(base, exponent):
    result = jnp.float32(1.0)
    value = base
    for bit in range(31):
        factor = value if value > 1e-37 else 0.0
        result = jnp.where((exponent >> bit) & 1 == 1, result * jnp.float32(factor), result)
        value = value * value
    return result


def adam_step(weight, mean, square, gradient, factor, first_scale, second_scale):
    scaled = factor * gradient
    mean_new = beta_first * mean + (1.0 - beta_first) * scaled
    square_new = beta_second * square + (1.0 - beta_second) * scaled * scaled
    mean_hat = mean_new * first_scale
    square_hat = square_new * second_scale
    weight_new = weight - learn_rate * (
        mean_hat / (jnp.sqrt(square_hat) + adam_epsilon) + decay_rate * weight
    )
    return weight_new, mean_new, square_new


def kernel(
    levels, experts, pieces, per_holder,
    grad_hbm, w_hbm, m_hbm, v_hbm, eg_hbm, ew_hbm, hm_hbm, hs_hbm,
    count_ref, holder_ref, slot_ref, step_ref,
    ow_ref, om_ref, ov_ref, oew_ref, oem_ref, oes_ref,
    grad, pair_out, local, recv, w_in, m_in, v_in, eg, ew, hm, hs,
    out_mean, out_square, in_mean, in_square, own_mean, own_square, part, parts,
    grad_sem, load_sem, pair_send, pair_recv, link_send, link_recv,
    mom_send, mom_recv, part_send, part_recv,
):
    dp = lax.axis_index("dp")
    me = lax.axis_index("expert")
    z = dp // CORES
    core = dp % CORES
    other = 1 - core
    partner = z * CORES + other
    upper = 2 * z >= levels
    maxb = holder_ref.shape[1]
    total_pieces = levels * pieces
    devices = levels * CORES * experts

    def level_of(j):
        return jnp.where(upper, j, levels - 1 - j)

    def grad_load(j):
        d = level_of(j)
        return pltpu.make_async_copy(grad_hbm.at[d], grad.at[d], grad_sem.at[j])

    for j in range(levels):
        grad_load(j).start()
    loads = [
        pltpu.make_async_copy(a, b, load_sem.at[i])
        for i, (a, b) in enumerate(
            ((hm_hbm, hm), (hs_hbm, hs), (eg_hbm, eg), (ew_hbm, ew), (w_hbm, w_in), (m_hbm, m_in), (v_hbm, v_in))
        )
    ]
    for load in loads:
        load.start()

    barrier = pltpu.get_barrier_semaphore()
    pl.semaphore_signal(barrier, inc=1, device_id=(partner, me), device_id_type=MESH)
    for off in range(1, experts):
        pl.semaphore_signal(barrier, inc=1, device_id=(dp, lax.rem(me + off, experts)), device_id_type=MESH)

    @pl.when(z > 0)
    def _():
        pl.semaphore_signal(barrier, inc=1, device_id=(dp - CORES, me), device_id_type=MESH)

    @pl.when(z < levels - 1)
    def _():
        pl.semaphore_signal(barrier, inc=1, device_id=(dp + CORES, me), device_id_type=MESH)

    near = jnp.where(z > 0, 1, 0) + jnp.where(z < levels - 1, 1, 0)
    pl.semaphore_wait(barrier, experts + near)

    def pair_copy(d, p):
        return pltpu.make_async_remote_copy(
            src_ref=pair_out.at[d, p], dst_ref=local.at[d, p],
            send_sem=pair_send.at[d * pieces + p], recv_sem=pair_recv.at[d * pieces + p],
            device_id=(partner, me), device_id_type=MESH,
        )

    def link_copy(way, d, p, src):
        return pltpu.make_async_remote_copy(
            src_ref=src, dst_ref=recv.at[way, d, p],
            send_sem=link_send.at[way, d * pieces + p], recv_sem=link_recv.at[way, d * pieces + p],
            device_id=(jnp.where(way == 0, dp + CORES, dp - CORES), me), device_id_type=MESH,
        )

    def give(j):
        grad_load(j).wait()
        d = level_of(j)

        @pl.loop(0, pieces)
        def _(p):
            pair_out[d, p] = grad[d, other, p].astype(jnp.float32)
            pair_copy(d, p).start()

    way_out = jnp.where(upper, 1, 0)
    at_end = (z == 0) | (z == levels - 1)

    def take(j):
        d = level_of(j)

        @pl.loop(0, pieces)
        def _(p):
            pair_copy(d, p).wait_recv()
            local[d, p] = local[d, p] + grad[d, core, p].astype(jnp.float32)

            @pl.when(at_end & (d != z))
            def _():
                link_copy(way_out, d, p, local.at[d, p]).start()

    give(0)

    @pl.loop(0, levels)
    def _(j):
        @pl.when(j + 1 < levels)
        def _():
            give(j + 1)

        take(j)

    loads[0].wait()
    loads[1].wait()

    def moment_copy(which, src, dst, target, source):
        return pltpu.make_async_remote_copy(
            src_ref=src.at[target], dst_ref=dst.at[source],
            send_sem=mom_send.at[which, target], recv_sem=mom_recv.at[which, source],
            device_id=(dp, target), device_id_type=MESH,
        )

    def picks(owner):
        rank = jnp.int32(0)
        chosen = [jnp.int32(0)] * per_holder
        for b in range(maxb):
            mine = (holder_ref[owner, b] == me) & (b < count_ref[owner])
            for q in range(per_holder):
                chosen[q] = jnp.where(mine & (rank == q), slot_ref[owner, b], chosen[q])
            rank = rank + jnp.where(mine, 1, 0)
        return chosen

    for q, slot in enumerate(picks(me)):
        in_mean[me, pl.ds(q, 1), :] = hm[pl.ds(slot, 1), :]
        in_square[me, pl.ds(q, 1), :] = hs[pl.ds(slot, 1), :]

    @pl.loop(1, experts)
    def _(off):
        owner = lax.rem(me + off, experts)
        for q, slot in enumerate(picks(owner)):
            out_mean[owner, pl.ds(q, 1), :] = hm[pl.ds(slot, 1), :]
            out_square[owner, pl.ds(q, 1), :] = hs[pl.ds(slot, 1), :]
        moment_copy(0, out_mean, in_mean, owner, me).start()
        moment_copy(1, out_square, in_square, owner, me).start()

    def forward(way, k):
        j = k // pieces
        p = k % pieces
        d = jnp.where(way == 0, levels - 1 - j, j)
        ahead = jnp.where(way == 0, (d > z) & (z > 0), (d < z) & (z < levels - 1))

        @pl.when(ahead)
        def _():
            copy = link_copy(way, d, p, recv.at[way, d, p])
            copy.wait_recv()
            recv[way, d, p] = recv[way, d, p] + local[d, p]
            copy.start()

    @pl.loop(0, total_pieces + LAG)
    def _(s):
        @pl.when(s < total_pieces)
        def _():
            forward(way_out, s)

        @pl.when(s >= LAG)
        def _():
            forward(1 - way_out, s - LAG)

    @pl.loop(1, experts)
    def _(off):
        source = lax.rem(me + off, experts)
        moment_copy(0, out_mean, in_mean, source, source).wait()
        moment_copy(1, out_square, in_square, source, source).wait()

    owned = count_ref[me]
    for b in range(maxb):
        holder = holder_ref[me, b]
        rank = jnp.int32(0)
        for earlier in range(b):
            rank = rank + jnp.where((holder_ref[me, earlier] == holder) & (earlier < owned), 1, 0)
        rank = jnp.minimum(rank, per_holder - 1)
        own_mean[pl.ds(b, 1), :] = in_mean[holder, pl.ds(rank, 1), :]
        own_square[pl.ds(b, 1), :] = in_square[holder, pl.ds(rank, 1), :]
    for load in loads[2:]:
        load.wait()
    width = eg.shape[1]
    live = lax.broadcasted_iota(jnp.int32, (maxb, 128), 0) < owned
    acc = jnp.zeros((maxb, 128), jnp.float32)
    for i in range(width // 128):
        g = eg[:, pl.ds(i * 128, 128)]
        acc = acc + jnp.where(live, g * g, 0.0)
    row = jnp.sum(acc, axis=0, keepdims=True)

    def finish(p, row):
        @pl.when(z < levels - 1)
        def _():
            link_copy(1, z, p, recv.at[1, z, p]).wait_recv()
            local[z, p] = local[z, p] + recv[1, z, p]

        @pl.when(z > 0)
        def _():
            link_copy(0, z, p, recv.at[0, z, p]).wait_recv()
            local[z, p] = local[z, p] + recv[0, z, p]

        g = local[z, p]
        col = jnp.sum(g * g, axis=0, keepdims=True)
        for i in range(g.shape[1] // 128):
            row = row + col[:, i * 128:(i + 1) * 128]
        return row

    row = lax.fori_loop(0, pieces, finish, row)

    index = dp * experts + me
    part[...] = row
    parts[index] = row

    def part_copy(off):
        target = lax.rem(index + off, devices)
        return pltpu.make_async_remote_copy(
            src_ref=part, dst_ref=parts.at[index],
            send_sem=part_send.at[off], recv_sem=part_recv,
            device_id=(target // experts, lax.rem(target, experts)), device_id_type=MESH,
        )

    @pl.loop(1, devices)
    def _(off):
        part_copy(off).start()

    step = step_ref[0]
    one = jnp.ones((1, 1), jnp.float32)
    first_scale = 1.0 / (one * (1.0 - power(beta_first, step)))
    second_scale = 1.0 / (one * (1.0 - power(beta_second, step)))
    others = parts.at[pl.ds(0, devices - 1)]
    pltpu.make_async_copy(others, others, part_recv).wait()
    total = jnp.sum(jnp.sum(parts[...], axis=0), axis=1, keepdims=True)
    factor = jnp.minimum(1.0, clip_norm / (jnp.sqrt(total) + 1e-06))

    @pl.loop(0, pieces)
    def _(p):
        w_new, m_new, v_new = adam_step(
            w_in[p], m_in[p], v_in[p], local[z, p], factor, first_scale, second_scale
        )
        ow_ref[p] = w_new
        om_ref[p] = m_new
        ov_ref[p] = v_new

    for i in range(width // 128):
        cols = pl.ds(i * 128, 128)
        w_old = ew[:, cols]
        w_new, m_new, v_new = adam_step(
            w_old, jnp.where(live, own_mean[:, cols], 0.0), jnp.where(live, own_square[:, cols], 0.0),
            eg[:, cols], factor, first_scale, second_scale,
        )
        oew_ref[:, cols] = jnp.where(live, w_new, w_old)
        oem_ref[:, cols] = jnp.where(live, m_new, 0.0)
        oes_ref[:, cols] = jnp.where(live, v_new, 0.0)

    @pl.loop(1, devices)
    def _(off):
        part_copy(off).wait_send()

    @pl.loop(0, total_pieces)
    def _(k):
        d = k // pieces
        p = k % pieces
        pair_copy(d, p).wait_send()

        @pl.when(d > z)
        def _():
            link_copy(0, d, p, local.at[d, p]).wait_send()

        @pl.when(d < z)
        def _():
            link_copy(1, d, p, local.at[d, p]).wait_send()


def piece_rows(rows):
    for size in range(96, 0, -16):
        if rows % size == 0:
            return size
    return rows


def make_body(mesh):
    n_dp = mesh.shape["dp"]
    experts = mesh.shape["expert"]
    levels = n_dp // CORES

    def body(ag, aw, am, av, eg, ew, hm, hs, count, holder, slot, step):
        depth, cols = ag.shape[1], ag.shape[2]
        rows = depth // n_dp
        size = piece_rows(rows)
        pieces = rows // size
        maxb, width = eg.shape[2], eg.shape[3]
        slots = hm.shape[1]
        per_holder = max(1, maxb // experts)
        f32 = jnp.float32
        own = (pieces, size, cols)
        k = levels * pieces
        dma = pltpu.SemaphoreType.DMA
        hbm = pl.BlockSpec(memory_space=pltpu.HBM)
        smem = pl.BlockSpec(memory_space=pltpu.SMEM)
        vmem = pl.BlockSpec(memory_space=pltpu.VMEM)
        outs = pl.pallas_call(
            functools.partial(kernel, levels, experts, pieces, per_holder),
            out_shape=[jax.ShapeDtypeStruct(own, f32)] * 3 + [jax.ShapeDtypeStruct((maxb, width), f32)] * 3,
            in_specs=[hbm] * 8 + [smem] * 4,
            out_specs=[vmem] * 6,
            scratch_shapes=[
                pltpu.VMEM((levels, CORES, pieces, size, cols), ag.dtype),
                pltpu.VMEM((levels, pieces, size, cols), f32),
                pltpu.VMEM((levels, pieces, size, cols), f32),
                pltpu.VMEM((2, levels, pieces, size, cols), f32),
                pltpu.VMEM(own, f32), pltpu.VMEM(own, f32), pltpu.VMEM(own, f32),
                pltpu.VMEM((maxb, width), f32), pltpu.VMEM((maxb, width), f32),
                pltpu.VMEM((slots, width), f32), pltpu.VMEM((slots, width), f32),
                pltpu.VMEM((experts, per_holder, width), f32), pltpu.VMEM((experts, per_holder, width), f32),
                pltpu.VMEM((experts, per_holder, width), f32), pltpu.VMEM((experts, per_holder, width), f32),
                pltpu.VMEM((maxb, width), f32), pltpu.VMEM((maxb, width), f32),
                pltpu.VMEM((1, 128), f32), pltpu.VMEM((n_dp * experts, 1, 128), f32),
                dma((levels,)), dma((7,)), dma((k,)), dma((k,)), dma((2, k)), dma((2, k)),
                dma((2, experts)), dma((2, experts)), dma((n_dp * experts,)), dma(()),
            ],
            compiler_params=pltpu.CompilerParams(
                collective_id=0, has_side_effects=True, vmem_limit_bytes=40 * 1024 * 1024
            ),
        )(
            ag.reshape(levels, CORES, pieces, size, cols),
            aw.reshape(own), am.reshape(own), av.reshape(own),
            eg[0, 0], ew[0, 0], hm[0], hs[0], count, holder, slot, step,
        )
        return tuple(o.reshape(rows, cols) for o in outs[:3]) + tuple(o[None, None] for o in outs[3:])

    return body


def solution(mesh):
    matrix = P("dp", "expert")
    blocks = P("dp", "expert", None, None)
    held = P("dp", "expert", None)
    return jax.shard_map(
        make_body(mesh),
        mesh=mesh,
        in_specs=(P("dp", None, "expert"), matrix, matrix, matrix, blocks, blocks, held, held, P(), P(), P(), P()),
        out_specs=(matrix, matrix, matrix, blocks, blocks, blocks),
        check_vma=False,
    )
```

```python
import functools

import jax
import jax.numpy as jnp
from jax import lax
from jax.experimental import pallas as pl
from jax.experimental.pallas import tpu as pltpu
from jax.sharding import PartitionSpec as P

MESH = pl.DeviceIdType.MESH
CORES = 2
LAG = 3
LIMIT = 40 * 1024 * 1024

beta_first = 0.9
beta_second = 0.95
learn_rate = 0.1
decay_rate = 0.1
adam_epsilon = 1e-08
clip_norm = 1.0


def power(base, exponent):
    result = jnp.float32(1.0)
    value = base
    for bit in range(31):
        factor = value if value > 1e-37 else 0.0
        result = jnp.where((exponent >> bit) & 1 == 1, result * jnp.float32(factor), result)
        value = value * value
    return result


def adam_step(weight, mean, square, gradient, factor, first_scale, second_scale):
    scaled = factor * gradient
    mean_new = beta_first * mean + (1.0 - beta_first) * scaled
    square_new = beta_second * square + (1.0 - beta_second) * scaled * scaled
    mean_hat = mean_new * first_scale
    square_hat = square_new * second_scale
    weight_new = weight - learn_rate * (
        mean_hat / (jnp.sqrt(square_hat) + adam_epsilon) + decay_rate * weight
    )
    return weight_new, mean_new, square_new


def kernel(
    levels, experts, pieces, per_holder,
    grad_hbm, eg_hbm, hm_hbm, hs_hbm, count_hbm, holder_hbm, slot_hbm, step_ref,
    sum_ref, own_mean, own_square, scale_ref, live_ref,
    grad, pair_out, local, recv, eg, hm, hs,
    out_mean, out_square, in_mean, in_square, part, parts, count_ref, holder_ref, slot_ref,
    grad_sem, load_sem, pair_send, pair_recv, link_send, link_recv,
    mom_send, mom_recv, part_send, part_recv,
):
    dp = lax.axis_index("dp")
    me = lax.axis_index("expert")
    z = dp // CORES
    core = dp % CORES
    other = 1 - core
    partner = z * CORES + other
    upper = 2 * z >= levels
    maxb = holder_ref.shape[1]
    total_pieces = levels * pieces
    devices = levels * CORES * experts

    def level_of(j):
        return jnp.where(upper, j, levels - 1 - j)

    def grad_load(j):
        d = level_of(j)
        return pltpu.make_async_copy(grad_hbm.at[d], grad.at[d], grad_sem.at[j])

    for j in range(levels):
        grad_load(j).start()
    loads = [
        pltpu.make_async_copy(a, b, load_sem.at[i])
        for i, (a, b) in enumerate(
            (
                (count_hbm, count_ref), (holder_hbm, holder_ref), (slot_hbm, slot_ref),
                (hm_hbm, hm), (hs_hbm, hs), (eg_hbm, eg),
            )
        )
    ]
    for load in loads:
        load.start()

    barrier = pltpu.get_barrier_semaphore()
    pl.semaphore_signal(barrier, inc=1, device_id=(partner, me), device_id_type=MESH)
    for off in range(1, experts):
        pl.semaphore_signal(barrier, inc=1, device_id=(dp, lax.rem(me + off, experts)), device_id_type=MESH)

    @pl.when(z > 0)
    def _():
        pl.semaphore_signal(barrier, inc=1, device_id=(dp - CORES, me), device_id_type=MESH)

    @pl.when(z < levels - 1)
    def _():
        pl.semaphore_signal(barrier, inc=1, device_id=(dp + CORES, me), device_id_type=MESH)

    first = level_of(0)
    grad_load(0).wait()

    @pl.loop(0, pieces)
    def _(p):
        pair_out[first, p] = grad[first, other, p].astype(jnp.float32)

    near = jnp.where(z > 0, 1, 0) + jnp.where(z < levels - 1, 1, 0)
    pl.semaphore_wait(barrier, experts + near)

    def pair_copy(d, p):
        return pltpu.make_async_remote_copy(
            src_ref=pair_out.at[d, p], dst_ref=local.at[d, p],
            send_sem=pair_send.at[d * pieces + p], recv_sem=pair_recv.at[d * pieces + p],
            device_id=(partner, me), device_id_type=MESH,
        )

    def link_copy(way, d, p, src):
        return pltpu.make_async_remote_copy(
            src_ref=src, dst_ref=recv.at[way, d, p],
            send_sem=link_send.at[way, d * pieces + p], recv_sem=link_recv.at[way, d * pieces + p],
            device_id=(jnp.where(way == 0, dp + CORES, dp - CORES), me), device_id_type=MESH,
        )

    def give(j):
        grad_load(j).wait()
        d = level_of(j)

        @pl.loop(0, pieces)
        def _(p):
            pair_out[d, p] = grad[d, other, p].astype(jnp.float32)
            pair_copy(d, p).start()

    way_out = jnp.where(upper, 1, 0)
    at_end = (z == 0) | (z == levels - 1)

    def take(j):
        d = level_of(j)

        @pl.loop(0, pieces)
        def _(p):
            pair_copy(d, p).wait_recv()
            local[d, p] = local[d, p] + grad[d, core, p].astype(jnp.float32)

            @pl.when(at_end & (d != z))
            def _():
                link_copy(way_out, d, p, local.at[d, p]).start()

    @pl.loop(0, pieces)
    def _(p):
        pair_copy(first, p).start()

    @pl.loop(0, levels)
    def _(j):
        @pl.when(j + 1 < levels)
        def _():
            give(j + 1)

        take(j)

    for load in loads[:5]:
        load.wait()

    def moment_copy(which, src, dst, target, source):
        return pltpu.make_async_remote_copy(
            src_ref=src.at[target], dst_ref=dst.at[source],
            send_sem=mom_send.at[which, target], recv_sem=mom_recv.at[which, source],
            device_id=(dp, target), device_id_type=MESH,
        )

    def picks(owner):
        rank = jnp.int32(0)
        chosen = [jnp.int32(0)] * per_holder
        for b in range(maxb):
            mine = (holder_ref[owner, b] == me) & (b < count_ref[owner])
            for q in range(per_holder):
                chosen[q] = jnp.where(mine & (rank == q), slot_ref[owner, b], chosen[q])
            rank = rank + jnp.where(mine, 1, 0)
        return chosen

    for q, slot in enumerate(picks(me)):
        in_mean[me, pl.ds(q, 1), :] = hm[pl.ds(slot, 1), :]
        in_square[me, pl.ds(q, 1), :] = hs[pl.ds(slot, 1), :]

    @pl.loop(1, experts)
    def _(off):
        owner = lax.rem(me + off, experts)
        for q, slot in enumerate(picks(owner)):
            out_mean[owner, pl.ds(q, 1), :] = hm[pl.ds(slot, 1), :]
            out_square[owner, pl.ds(q, 1), :] = hs[pl.ds(slot, 1), :]
        moment_copy(0, out_mean, in_mean, owner, me).start()
        moment_copy(1, out_square, in_square, owner, me).start()

    def forward(way, k):
        j = k // pieces
        p = k % pieces
        d = jnp.where(way == 0, levels - 1 - j, j)
        ahead = jnp.where(way == 0, (d > z) & (z > 0), (d < z) & (z < levels - 1))

        @pl.when(ahead)
        def _():
            copy = link_copy(way, d, p, recv.at[way, d, p])
            copy.wait_recv()
            recv[way, d, p] = recv[way, d, p] + local[d, p]
            copy.start()

    @pl.loop(0, total_pieces + LAG)
    def _(s):
        @pl.when(s < total_pieces)
        def _():
            forward(way_out, s)

        @pl.when(s >= LAG)
        def _():
            forward(1 - way_out, s - LAG)

    @pl.loop(1, experts)
    def _(off):
        source = lax.rem(me + off, experts)
        moment_copy(0, out_mean, in_mean, source, source).wait()
        moment_copy(1, out_square, in_square, source, source).wait()

    owned = count_ref[me]
    for b in range(maxb):
        holder = holder_ref[me, b]
        rank = jnp.int32(0)
        for earlier in range(b):
            rank = rank + jnp.where((holder_ref[me, earlier] == holder) & (earlier < owned), 1, 0)
        rank = jnp.minimum(rank, per_holder - 1)
        own_mean[pl.ds(b, 1), :] = in_mean[holder, pl.ds(rank, 1), :]
        own_square[pl.ds(b, 1), :] = in_square[holder, pl.ds(rank, 1), :]
    loads[5].wait()
    width = eg.shape[1]
    live = lax.broadcasted_iota(jnp.int32, (maxb, 128), 0) < owned
    acc = jnp.zeros((maxb, 128), jnp.float32)
    for i in range(width // 128):
        g = eg[:, pl.ds(i * 128, 128)]
        acc = acc + jnp.where(live, g * g, 0.0)
    row = jnp.sum(acc, axis=0, keepdims=True)
    live_ref[...] = jnp.where(live, 1.0, 0.0)
    step = step_ref[0]
    one = jnp.ones((1, 128), jnp.float32)
    scale_ref[1:2] = 1.0 / (one * (1.0 - power(beta_first, step)))
    scale_ref[2:3] = 1.0 / (one * (1.0 - power(beta_second, step)))

    def finish(p, row):
        sum_ref[p] = local[z, p]

        @pl.when(z < levels - 1)
        def _():
            link_copy(1, z, p, recv.at[1, z, p]).wait_recv()

            @pl.when(z > 0)
            def _():
                link_copy(0, z, p, recv.at[0, z, p]).wait_recv()
                sum_ref[p] = local[z, p] + (recv[0, z, p] + recv[1, z, p])

            @pl.when(z == 0)
            def _():
                sum_ref[p] = local[z, p] + recv[1, z, p]

        @pl.when((z == levels - 1) & (z > 0))
        def _():
            link_copy(0, z, p, recv.at[0, z, p]).wait_recv()
            sum_ref[p] = local[z, p] + recv[0, z, p]

        g = sum_ref[p]
        col = jnp.sum(g * g, axis=0, keepdims=True)
        for i in range(g.shape[1] // 128):
            row = row + col[:, i * 128:(i + 1) * 128]
        return row

    row = lax.fori_loop(0, pieces, finish, row)

    index = dp * experts + me
    part[...] = row
    parts[index] = row

    def part_copy(off):
        target = lax.rem(index + off, devices)
        return pltpu.make_async_remote_copy(
            src_ref=part, dst_ref=parts.at[index],
            send_sem=part_send.at[off], recv_sem=part_recv,
            device_id=(target // experts, lax.rem(target, experts)), device_id_type=MESH,
        )

    @pl.loop(1, devices)
    def _(off):
        part_copy(off).start()

    @pl.loop(0, total_pieces)
    def _(k):
        d = k // pieces
        p = k % pieces
        pair_copy(d, p).wait_send()

        @pl.when(d > z)
        def _():
            link_copy(0, d, p, local.at[d, p]).wait_send()

        @pl.when(d < z)
        def _():
            link_copy(1, d, p, local.at[d, p]).wait_send()

    others = parts.at[pl.ds(0, devices - 1)]
    pltpu.make_async_copy(others, others, part_recv).wait()
    total = jnp.sum(jnp.sum(parts[...], axis=0), axis=1, keepdims=True)
    scale_ref[0:1] = jnp.broadcast_to(jnp.minimum(1.0, clip_norm / (jnp.sqrt(total) + 1e-06)), (1, 128))

    @pl.loop(1, devices)
    def _(off):
        part_copy(off).wait_send()


def update(
    w_in, m_in, v_in, sums, eg, ew, own_mean, own_square, scale_ref, live_ref,
    ow_hbm, om_hbm, ov_hbm, oew_hbm, oem_hbm, oes_hbm,
    ow, om, ov, oew, oem, oes, sem, expert_sem,
):
    factor = scale_ref[0:1, 0:1]
    first_scale = scale_ref[1:2, 0:1]
    second_scale = scale_ref[2:3, 0:1]
    pieces = w_in.shape[0]
    triples = ((ow, ow_hbm), (om, om_hbm), (ov, ov_hbm))

    def put(i, p):
        src, dst = triples[i]
        return pltpu.make_async_copy(src.at[p], dst.at[p], sem.at[i, p])

    @pl.loop(0, pieces)
    def _(p):
        w_new, m_new, v_new = adam_step(
            w_in[p], m_in[p], v_in[p], sums[p], factor, first_scale, second_scale
        )
        ow[p] = w_new
        om[p] = m_new
        ov[p] = v_new
        for i in range(3):
            put(i, p).start()

    maxb, width = eg.shape
    live = live_ref[...] > 0.5
    for i in range(width // 128):
        cols = pl.ds(i * 128, 128)
        w_old = ew[:, cols]
        w_new, m_new, v_new = adam_step(
            w_old, jnp.where(live, own_mean[:, cols], 0.0), jnp.where(live, own_square[:, cols], 0.0),
            eg[:, cols], factor, first_scale, second_scale,
        )
        oew[:, cols] = jnp.where(live, w_new, w_old)
        oem[:, cols] = jnp.where(live, m_new, 0.0)
        oes[:, cols] = jnp.where(live, v_new, 0.0)
    rest = [
        pltpu.make_async_copy(a, b, expert_sem.at[i])
        for i, (a, b) in enumerate(((oew, oew_hbm), (oem, oem_hbm), (oes, oes_hbm)))
    ]
    for copy in rest:
        copy.start()

    @pl.loop(0, pieces)
    def _(p):
        for i in range(3):
            put(i, p).wait()

    for copy in rest:
        copy.wait()


def piece_rows(rows):
    for size in range(96, 0, -16):
        if rows % size == 0:
            return size
    return rows


def make_body(mesh):
    n_dp = mesh.shape["dp"]
    experts = mesh.shape["expert"]
    levels = n_dp // CORES

    def body(ag, aw, am, av, eg, ew, hm, hs, count, holder, slot, step):
        depth, cols = ag.shape[1], ag.shape[2]
        rows = depth // n_dp
        size = piece_rows(rows)
        pieces = rows // size
        maxb, width = eg.shape[2], eg.shape[3]
        slots = hm.shape[1]
        per_holder = max(1, maxb // experts)
        f32 = jnp.float32
        own = (pieces, size, cols)
        k = levels * pieces
        dma = pltpu.SemaphoreType.DMA
        hbm = pl.BlockSpec(memory_space=pltpu.HBM)
        vmem = pl.BlockSpec(memory_space=pltpu.VMEM)
        blocks = (maxb, width)
        shape = jax.ShapeDtypeStruct
        moved = (experts, per_holder, width)
        sums, own_mean, own_square, scales, live = pl.pallas_call(
            functools.partial(kernel, levels, experts, pieces, per_holder),
            out_shape=[pltpu.VMEM(s, f32) for s in (own, blocks, blocks, (3, 128), (maxb, 128))],
            in_specs=[hbm] * 7 + [pl.BlockSpec(memory_space=pltpu.SMEM)],
            out_specs=[vmem] * 5,
            scratch_shapes=[
                pltpu.VMEM((levels, CORES, pieces, size, cols), ag.dtype),
                pltpu.VMEM((levels, pieces, size, cols), f32),
                pltpu.VMEM((levels, pieces, size, cols), f32),
                pltpu.VMEM((2, levels, pieces, size, cols), f32),
                pltpu.VMEM(blocks, f32),
                pltpu.VMEM((slots, width), f32), pltpu.VMEM((slots, width), f32),
                pltpu.VMEM(moved, f32), pltpu.VMEM(moved, f32),
                pltpu.VMEM(moved, f32), pltpu.VMEM(moved, f32),
                pltpu.VMEM((1, 128), f32), pltpu.VMEM((n_dp * experts, 1, 128), f32),
                pltpu.SMEM(count.shape, jnp.int32), pltpu.SMEM(holder.shape, jnp.int32),
                pltpu.SMEM(slot.shape, jnp.int32),
                dma((levels,)), dma((6,)), dma((k,)), dma((k,)), dma((2, k)), dma((2, k)),
                dma((2, experts)), dma((2, experts)), dma((n_dp * experts,)), dma(()),
            ],
            compiler_params=pltpu.CompilerParams(
                collective_id=0, has_side_effects=True, vmem_limit_bytes=LIMIT
            ),
        )(
            *(pltpu.with_memory_space_constraint(x, pltpu.HBM) for x in (
                ag.reshape(levels, CORES, pieces, size, cols), eg[0, 0], hm[0], hs[0],
                count, holder, slot,
            )),
            step,
        )
        outs = pl.pallas_call(
            update,
            out_shape=[shape(own, f32)] * 3 + [shape(blocks, f32)] * 3,
            in_specs=[vmem] * 10,
            out_specs=[hbm] * 6,
            scratch_shapes=[pltpu.VMEM(own, f32)] * 3 + [pltpu.VMEM(blocks, f32)] * 3 + [dma((3, pieces)), dma((3,))],
            compiler_params=pltpu.CompilerParams(vmem_limit_bytes=16 * 1024 * 1024),
        )(
            aw.reshape(own), am.reshape(own), av.reshape(own), sums,
            eg[0, 0], ew[0, 0], own_mean, own_square, scales, live,
        )
        return tuple(o.reshape(rows, cols) for o in outs[:3]) + tuple(o[None, None] for o in outs[3:])

    return body


def solution(mesh):
    matrix = P("dp", "expert")
    blocks = P("dp", "expert", None, None)
    held = P("dp", "expert", None)
    return jax.shard_map(
        make_body(mesh),
        mesh=mesh,
        in_specs=(P("dp", None, "expert"), matrix, matrix, matrix, blocks, blocks, held, held, P(), P(), P(), P()),
        out_specs=(matrix, matrix, matrix, blocks, blocks, blocks),
        check_vma=False,
    )
```

```python
import functools

import jax
import jax.numpy as jnp
from jax import lax
from jax.experimental import pallas as pl
from jax.experimental.pallas import tpu as pltpu
from jax.sharding import PartitionSpec as P

MESH = pl.DeviceIdType.MESH
CORES = 2
LAG = 1
LIMIT = 40 * 1024 * 1024

beta_first = 0.9
beta_second = 0.95
learn_rate = 0.1
decay_rate = 0.1
adam_epsilon = 1e-08
clip_norm = 1.0


def power(base, exponent):
    result = jnp.float32(1.0)
    value = base
    for bit in range(31):
        factor = value if value > 1e-37 else 0.0
        result = jnp.where((exponent >> bit) & 1 == 1, result * jnp.float32(factor), result)
        value = value * value
    return result


def adam_step(weight, mean, square, gradient, factor, first_scale, second_scale):
    scaled = factor * gradient
    mean_new = beta_first * mean + (1.0 - beta_first) * scaled
    square_new = beta_second * square + (1.0 - beta_second) * scaled * scaled
    mean_hat = mean_new * first_scale
    square_hat = square_new * second_scale
    weight_new = weight - learn_rate * (
        mean_hat / (jnp.sqrt(square_hat) + adam_epsilon) + decay_rate * weight
    )
    return weight_new, mean_new, square_new


def kernel(
    levels, experts, pieces, per_holder,
    grad_hbm, eg_hbm, ew_hbm, w_hbm, m_hbm, v_hbm, hm_hbm, hs_hbm, count_hbm, holder_hbm, slot_hbm, step_ref,
    sum_ref, own_mean, own_square, scale_ref, live_ref, eg, ew, w_in, m_in, v_in,
    grad, pair_out, local, recv, hm, hs,
    out_mean, out_square, in_mean, in_square, part, parts, count_ref, holder_ref, slot_ref,
    grad_sem, load_sem, pair_send, pair_recv, link_send, link_recv,
    mom_send, mom_recv, part_send, part_recv,
):
    dp = lax.axis_index("dp")
    me = lax.axis_index("expert")
    z = dp // CORES
    core = dp % CORES
    other = 1 - core
    partner = z * CORES + other
    upper = 2 * z >= levels
    maxb = holder_ref.shape[1]
    total_pieces = levels * pieces
    devices = levels * CORES * experts

    def level_of(j):
        return jnp.where(upper, j, levels - 1 - j)

    def grad_load(j):
        d = level_of(j)
        return pltpu.make_async_copy(grad_hbm.at[d], grad.at[d], grad_sem.at[j])

    for j in range(levels):
        grad_load(j).start()
    loads = [
        pltpu.make_async_copy(a, b, load_sem.at[i])
        for i, (a, b) in enumerate(
            (
                (count_hbm, count_ref), (holder_hbm, holder_ref), (slot_hbm, slot_ref),
                (hm_hbm, hm), (hs_hbm, hs), (eg_hbm, eg),
                (ew_hbm, ew), (w_hbm, w_in), (m_hbm, m_in), (v_hbm, v_in),
            )
        )
    ]
    barrier = pltpu.get_barrier_semaphore()
    pl.semaphore_signal(barrier, inc=1, device_id=(partner, me), device_id_type=MESH)
    for off in range(1, experts):
        pl.semaphore_signal(barrier, inc=1, device_id=(dp, lax.rem(me + off, experts)), device_id_type=MESH)

    @pl.when(z > 0)
    def _():
        pl.semaphore_signal(barrier, inc=1, device_id=(dp - CORES, me), device_id_type=MESH)

    @pl.when(z < levels - 1)
    def _():
        pl.semaphore_signal(barrier, inc=1, device_id=(dp + CORES, me), device_id_type=MESH)

    first = level_of(0)
    grad_load(0).wait()

    @pl.loop(0, pieces)
    def _(p):
        pair_out[first, p] = grad[first, other, p].astype(jnp.float32)

    near = jnp.where(z > 0, 1, 0) + jnp.where(z < levels - 1, 1, 0)
    pl.semaphore_wait(barrier, experts + near)

    def pair_copy(d, p):
        return pltpu.make_async_remote_copy(
            src_ref=pair_out.at[d, p], dst_ref=local.at[d, p],
            send_sem=pair_send.at[d * pieces + p], recv_sem=pair_recv.at[d * pieces + p],
            device_id=(partner, me), device_id_type=MESH,
        )

    def link_copy(way, d, p, src):
        return pltpu.make_async_remote_copy(
            src_ref=src, dst_ref=recv.at[way, d, p],
            send_sem=link_send.at[way, d * pieces + p], recv_sem=link_recv.at[way, d * pieces + p],
            device_id=(jnp.where(way == 0, dp + CORES, dp - CORES), me), device_id_type=MESH,
        )

    def give(j):
        grad_load(j).wait()
        d = level_of(j)

        @pl.loop(0, pieces)
        def _(p):
            pair_out[d, p] = grad[d, other, p].astype(jnp.float32)
            pair_copy(d, p).start()

    way_out = jnp.where(upper, 1, 0)
    at_end = (z == 0) | (z == levels - 1)

    def take(j):
        d = level_of(j)

        @pl.loop(0, pieces)
        def _(p):
            pair_copy(d, p).wait_recv()
            local[d, p] = local[d, p] + grad[d, core, p].astype(jnp.float32)

            @pl.when(at_end & (d != z))
            def _():
                link_copy(way_out, d, p, local.at[d, p]).start()

    @pl.loop(0, pieces)
    def _(p):
        pair_copy(first, p).start()

    for load in loads[:5]:
        load.start()

    @pl.loop(0, levels)
    def _(j):
        @pl.when(j + 1 < levels)
        def _():
            give(j + 1)

        take(j)

    for load in loads[5:]:
        load.start()
    for load in loads[:5]:
        load.wait()

    def moment_copy(which, src, dst, target, source):
        return pltpu.make_async_remote_copy(
            src_ref=src.at[target], dst_ref=dst.at[source],
            send_sem=mom_send.at[which, target], recv_sem=mom_recv.at[which, source],
            device_id=(dp, target), device_id_type=MESH,
        )

    def picks(owner):
        rank = jnp.int32(0)
        chosen = [jnp.int32(0)] * per_holder
        for b in range(maxb):
            mine = (holder_ref[owner, b] == me) & (b < count_ref[owner])
            for q in range(per_holder):
                chosen[q] = jnp.where(mine & (rank == q), slot_ref[owner, b], chosen[q])
            rank = rank + jnp.where(mine, 1, 0)
        return chosen

    for q, slot in enumerate(picks(me)):
        in_mean[me, pl.ds(q, 1), :] = hm[pl.ds(slot, 1), :]
        in_square[me, pl.ds(q, 1), :] = hs[pl.ds(slot, 1), :]

    @pl.loop(1, experts)
    def _(off):
        owner = lax.rem(me + off, experts)
        for q, slot in enumerate(picks(owner)):
            out_mean[owner, pl.ds(q, 1), :] = hm[pl.ds(slot, 1), :]
            out_square[owner, pl.ds(q, 1), :] = hs[pl.ds(slot, 1), :]
        moment_copy(0, out_mean, in_mean, owner, me).start()
        moment_copy(1, out_square, in_square, owner, me).start()

    def forward(way, k):
        j = k // pieces
        p = k % pieces
        d = jnp.where(way == 0, levels - 1 - j, j)
        ahead = jnp.where(way == 0, (d > z) & (z > 0), (d < z) & (z < levels - 1))

        @pl.when(ahead)
        def _():
            copy = link_copy(way, d, p, recv.at[way, d, p])
            copy.wait_recv()
            recv[way, d, p] = recv[way, d, p] + local[d, p]
            copy.start()

    @pl.loop(0, total_pieces + LAG)
    def _(s):
        @pl.when(s < total_pieces)
        def _():
            forward(way_out, s)

        @pl.when(s >= LAG)
        def _():
            forward(1 - way_out, s - LAG)

    @pl.loop(1, experts)
    def _(off):
        source = lax.rem(me + off, experts)
        moment_copy(0, out_mean, in_mean, source, source).wait()
        moment_copy(1, out_square, in_square, source, source).wait()

    owned = count_ref[me]
    for b in range(maxb):
        holder = holder_ref[me, b]
        rank = jnp.int32(0)
        for earlier in range(b):
            rank = rank + jnp.where((holder_ref[me, earlier] == holder) & (earlier < owned), 1, 0)
        rank = jnp.minimum(rank, per_holder - 1)
        own_mean[pl.ds(b, 1), :] = in_mean[holder, pl.ds(rank, 1), :]
        own_square[pl.ds(b, 1), :] = in_square[holder, pl.ds(rank, 1), :]
    for load in loads[5:]:
        load.wait()
    width = eg.shape[1]
    live = lax.broadcasted_iota(jnp.int32, (maxb, 128), 0) < owned
    acc = jnp.zeros((maxb, 128), jnp.float32)
    for i in range(width // 128):
        g = eg[:, pl.ds(i * 128, 128)]
        acc = acc + jnp.where(live, g * g, 0.0)
    row = jnp.sum(acc, axis=0, keepdims=True)
    live_ref[...] = jnp.where(live, 1.0, 0.0)
    step = step_ref[0]
    one = jnp.ones((1, 128), jnp.float32)
    scale_ref[1:2] = 1.0 / (one * (1.0 - power(beta_first, step)))
    scale_ref[2:3] = 1.0 / (one * (1.0 - power(beta_second, step)))

    def finish(p, row):
        sum_ref[p] = local[z, p]

        @pl.when(z < levels - 1)
        def _():
            link_copy(1, z, p, recv.at[1, z, p]).wait_recv()

            @pl.when(z > 0)
            def _():
                link_copy(0, z, p, recv.at[0, z, p]).wait_recv()
                sum_ref[p] = local[z, p] + (recv[0, z, p] + recv[1, z, p])

            @pl.when(z == 0)
            def _():
                sum_ref[p] = local[z, p] + recv[1, z, p]

        @pl.when((z == levels - 1) & (z > 0))
        def _():
            link_copy(0, z, p, recv.at[0, z, p]).wait_recv()
            sum_ref[p] = local[z, p] + recv[0, z, p]

        g = sum_ref[p]
        col = jnp.sum(g * g, axis=0, keepdims=True)
        for i in range(g.shape[1] // 128):
            row = row + col[:, i * 128:(i + 1) * 128]
        return row

    row = lax.fori_loop(0, pieces, finish, row)

    index = dp * experts + me
    part[...] = row
    parts[index] = row

    def part_copy(off):
        target = lax.rem(index + off, devices)
        return pltpu.make_async_remote_copy(
            src_ref=part, dst_ref=parts.at[index],
            send_sem=part_send.at[off], recv_sem=part_recv,
            device_id=(target // experts, lax.rem(target, experts)), device_id_type=MESH,
        )

    @pl.loop(1, devices)
    def _(off):
        part_copy(off).start()

    @pl.loop(0, total_pieces)
    def _(k):
        d = k // pieces
        p = k % pieces
        pair_copy(d, p).wait_send()

        @pl.when(d > z)
        def _():
            link_copy(0, d, p, local.at[d, p]).wait_send()

        @pl.when(d < z)
        def _():
            link_copy(1, d, p, local.at[d, p]).wait_send()

    others = parts.at[pl.ds(0, devices - 1)]
    pltpu.make_async_copy(others, others, part_recv).wait()
    total = jnp.sum(jnp.sum(parts[...], axis=0), axis=1, keepdims=True)
    scale_ref[0:1] = jnp.broadcast_to(jnp.minimum(1.0, clip_norm / (jnp.sqrt(total) + 1e-06)), (1, 128))

    @pl.loop(1, devices)
    def _(off):
        part_copy(off).wait_send()


def update(
    w_in, m_in, v_in, sums, eg, ew, own_mean, own_square, scale_ref, live_ref,
    ow_hbm, om_hbm, ov_hbm, oew_hbm, oem_hbm, oes_hbm,
    ow, om, ov, oew, oem, oes, sem, expert_sem,
):
    factor = scale_ref[0:1, 0:1]
    first_scale = scale_ref[1:2, 0:1]
    second_scale = scale_ref[2:3, 0:1]
    pieces = w_in.shape[0]
    triples = ((ow, ow_hbm), (om, om_hbm), (ov, ov_hbm))

    def put(i, p):
        src, dst = triples[i]
        return pltpu.make_async_copy(src.at[p], dst.at[p], sem.at[i, p])

    @pl.loop(0, pieces)
    def _(p):
        w_new, m_new, v_new = adam_step(
            w_in[p], m_in[p], v_in[p], sums[p], factor, first_scale, second_scale
        )
        ow[p] = w_new
        om[p] = m_new
        ov[p] = v_new
        for i in range(3):
            put(i, p).start()

    maxb, width = eg.shape
    live = live_ref[...] > 0.5
    for i in range(width // 128):
        cols = pl.ds(i * 128, 128)
        w_old = ew[:, cols]
        w_new, m_new, v_new = adam_step(
            w_old, jnp.where(live, own_mean[:, cols], 0.0), jnp.where(live, own_square[:, cols], 0.0),
            eg[:, cols], factor, first_scale, second_scale,
        )
        oew[:, cols] = jnp.where(live, w_new, w_old)
        oem[:, cols] = jnp.where(live, m_new, 0.0)
        oes[:, cols] = jnp.where(live, v_new, 0.0)
    rest = [
        pltpu.make_async_copy(a, b, expert_sem.at[i])
        for i, (a, b) in enumerate(((oew, oew_hbm), (oem, oem_hbm), (oes, oes_hbm)))
    ]
    for copy in rest:
        copy.start()

    @pl.loop(0, pieces)
    def _(p):
        for i in range(3):
            put(i, p).wait()

    for copy in rest:
        copy.wait()


def piece_rows(rows):
    for size in range(192, 0, -16):
        if rows % size == 0:
            return size
    return rows


def make_body(mesh):
    n_dp = mesh.shape["dp"]
    experts = mesh.shape["expert"]
    levels = n_dp // CORES

    def body(ag, aw, am, av, eg, ew, hm, hs, count, holder, slot, step):
        depth, cols = ag.shape[1], ag.shape[2]
        rows = depth // n_dp
        size = piece_rows(rows)
        pieces = rows // size
        maxb, width = eg.shape[2], eg.shape[3]
        slots = hm.shape[1]
        per_holder = max(1, maxb // experts)
        f32 = jnp.float32
        own = (pieces, size, cols)
        k = levels * pieces
        dma = pltpu.SemaphoreType.DMA
        hbm = pl.BlockSpec(memory_space=pltpu.HBM)
        vmem = pl.BlockSpec(memory_space=pltpu.VMEM)
        blocks = (maxb, width)
        shape = jax.ShapeDtypeStruct
        moved = (experts, per_holder, width)
        sums, own_mean, own_square, scales, live, eg_in, ew_in, w_in, m_in, v_in = pl.pallas_call(
            functools.partial(kernel, levels, experts, pieces, per_holder),
            out_shape=[pltpu.VMEM(s, f32) for s in (own, blocks, blocks, (3, 128), (maxb, 128), blocks, blocks, own, own, own)],
            in_specs=[hbm] * 11 + [pl.BlockSpec(memory_space=pltpu.SMEM)],
            out_specs=[vmem] * 10,
            scratch_shapes=[
                pltpu.VMEM((levels, CORES, pieces, size, cols), ag.dtype),
                pltpu.VMEM((levels, pieces, size, cols), f32),
                pltpu.VMEM((levels, pieces, size, cols), f32),
                pltpu.VMEM((2, levels, pieces, size, cols), f32),
                pltpu.VMEM((slots, width), f32), pltpu.VMEM((slots, width), f32),
                pltpu.VMEM(moved, f32), pltpu.VMEM(moved, f32),
                pltpu.VMEM(moved, f32), pltpu.VMEM(moved, f32),
                pltpu.VMEM((1, 128), f32), pltpu.VMEM((n_dp * experts, 1, 128), f32),
                pltpu.SMEM(count.shape, jnp.int32), pltpu.SMEM(holder.shape, jnp.int32),
                pltpu.SMEM(slot.shape, jnp.int32),
                dma((levels,)), dma((10,)), dma((k,)), dma((k,)), dma((2, k)), dma((2, k)),
                dma((2, experts)), dma((2, experts)), dma((n_dp * experts,)), dma(()),
            ],
            compiler_params=pltpu.CompilerParams(
                collective_id=0, has_side_effects=True, vmem_limit_bytes=LIMIT
            ),
        )(
            *(pltpu.with_memory_space_constraint(x, pltpu.HBM) for x in (
                ag.reshape(levels, CORES, pieces, size, cols), eg[0, 0], ew[0, 0],
                aw.reshape(own), am.reshape(own), av.reshape(own), hm[0], hs[0],
                count, holder, slot,
            )),
            step,
        )
        outs = pl.pallas_call(
            update,
            out_shape=[shape(own, f32)] * 3 + [shape(blocks, f32)] * 3,
            in_specs=[vmem] * 10,
            out_specs=[hbm] * 6,
            scratch_shapes=[pltpu.VMEM(own, f32)] * 3 + [pltpu.VMEM(blocks, f32)] * 3 + [dma((3, pieces)), dma((3,))],
            compiler_params=pltpu.CompilerParams(vmem_limit_bytes=16 * 1024 * 1024),
        )(
            w_in, m_in, v_in, sums, eg_in, ew_in, own_mean, own_square, scales, live,
        )
        return tuple(o.reshape(rows, cols) for o in outs[:3]) + tuple(o[None, None] for o in outs[3:])

    return body


def solution(mesh):
    matrix = P("dp", "expert")
    blocks = P("dp", "expert", None, None)
    held = P("dp", "expert", None)
    return jax.shard_map(
        make_body(mesh),
        mesh=mesh,
        in_specs=(P("dp", None, "expert"), matrix, matrix, matrix, blocks, blocks, held, held, P(), P(), P(), P()),
        out_specs=(matrix, matrix, matrix, blocks, blocks, blocks),
        check_vma=False,
    )
```
